32 devices in a mesh: row: 4 (over x, core), col: 2 (over y), dp: 4 (over z).
Axes of the slice: x: 2, y: 2, z: 4, core: 2. Of those that a mesh axis runs over, the one named last changes fastest.
Arguments:
- tokens: bfloat16 [16384, 768], P(('dp', 'col', 'row')), may hold values from -6 to 6
- encoded: bfloat16 [12000, 768], P(('dp', 'col', 'row')), may hold values from -6 to 6
- branch: int32 [8, 4], P(('dp', 'col')), may hold values from 512 to 1024
- cotangent: bfloat16 [16384, 768], P(('dp', 'col', 'row')), may hold values from -6 to 6
- gain_self: float32 [768], replicated, may hold values from 0.5 to 1.5
- self_query: bfloat16 [768, 768], P('col', 'row'), may hold values from -0.21875 to 0.21875
- self_key: bfloat16 [768, 768], P('col', 'row'), may hold values from -0.21875 to 0.21875
- self_value: bfloat16 [768, 768], P('col', 'row'), may hold values from -0.21875 to 0.21875
- self_out: bfloat16 [768, 768], P('row', 'col'), may hold values from -3 to 3
- gain_cross: float32 [768], replicated, may hold values from 0.5 to 1.5
- cross_query: bfloat16 [768, 768], P('col', 'row'), may hold values from -0.21875 to 0.21875
- cross_key: bfloat16 [768, 768], P('col', 'row'), may hold values from -0.21875 to 0.21875
- cross_value: bfloat16 [768, 768], P('col', 'row'), may hold values from -0.21875 to 0.21875
- cross_out: bfloat16 [768, 768], P('row', 'col'), may hold values from -4 to 4
- gain_hidden: float32 [768], replicated, may hold values from 0.5 to 1.5
- hidden_up: bfloat16 [768, 3072], P('col', 'row'), may hold values from -0.21875 to 0.21875
- hidden_down: bfloat16 [3072, 768], P('row', 'col'), may hold values from -0.109375 to 0.109375
- gain_final: float32 [768], replicated, may hold values from 0.5 to 1.5
Outputs:
- layer_out: bfloat16 [16384, 768], P(('dp', 'col', 'row'))
- grad_tokens: float32 [16384, 768], P(('dp', 'col', 'row'))
- grad_encoded: float32 [12000, 768], P(('dp', 'col', 'row'))
- grad_gain_self: float32 [768], replicated
- grad_self_query: float32 [768, 768], P('col', 'row')
- grad_self_key: float32 [768, 768], P('col', 'row')
- grad_self_value: float32 [768, 768], P('col', 'row')
- grad_self_out: float32 [768, 768], P('row', 'col')
- grad_gain_cross: float32 [768], replicated
- grad_cross_query: float32 [768, 768], P('col', 'row')
- grad_cross_key: float32 [768, 768], P('col', 'row')
- grad_cross_value: float32 [768, 768], P('col', 'row')
- grad_cross_out: float32 [768, 768], P('row', 'col')
- grad_gain_hidden: float32 [768], replicated
- grad_hidden_up: float32 [768, 3072], P('col', 'row')
- grad_hidden_down: float32 [3072, 768], P('row', 'col')
- grad_gain_final: float32 [768], replicated
The draws below stay inside these ranges and needn't reach their ends.
Inputs may be any that keep to these rules, and one draw needn't show every extreme that they name: Continuation j of family f sees the first branch[f, j] prompt positions.
All inputs are finite; a program needn't handle non-finite values.
Results may differ from the reference program's by a relative error of at most 0.025.
Values may be sent and summed in bfloat16 or wider, within the bound.
A program may use at most 192 MiB of HBM per device.

```python
import jax
import jax.numpy as jnp
from jax import lax

D = 768
HEAD_DIM = 64
FF = 3072
PROMPT = 1024
CONT = 256
NCONT = 4
FRAMES = 1500
FAMLEN = 2048
FAMILIES = 8
TOKENS = 16384
FRAMES_ALL = 12000


def plant(result, rng, smallest, top_value):
    longest = result.shape.index(max(result.shape))
    spots = []
    for shift in (0, 1):
        where = [jax.random.randint(jax.random.fold_in(rng, axis), (), 0, length) for axis, length in enumerate(result.shape)]
        where[longest] = (where[longest] + shift) % result.shape[longest]
        spots.append(tuple(where))
    return result.at[spots[0]].set(smallest).at[spots[1]].set(top_value)


def block_scale(stream_key, shape, cuts, least, largest):
    def one(position, parts):
        heights = jax.random.uniform(jax.random.fold_in(jax.random.fold_in(stream_key, 6), position), (parts,), jnp.float32, least / len(cuts), largest / len(cuts))
        return jnp.repeat(jnp.exp(heights), shape[position] // parts).reshape((-1,) + (1,) * (len(shape) - position - 1))

    factor_of = one(*cuts[0])
    for cut in cuts[1:]:
        factor_of = factor_of * one(*cut)
    return factor_of


def scatter_about(own_key, dims, spread, bound, cuts=(), kind=jnp.bfloat16):
    drawn = spread * jax.random.normal(own_key, dims, jnp.float32)
    if cuts:
        drawn = drawn * block_scale(own_key, dims, cuts, -0.22, 0.18)
    return jnp.clip(drawn, -bound, bound).astype(kind)


def setup_inputs(seed: int = 0) -> dict:
    key_list = jax.random.split(jax.random.key(seed), 19)
    tokens = scatter_about(key_list[0], (TOKENS, D), 1.0, 6.0, ((0, 32),))
    encoded = scatter_about(key_list[1], (FRAMES_ALL, D), 1.0, 6.0, ((0, 32),))
    branch = plant(jax.random.randint(key_list[2], (FAMILIES, NCONT), PROMPT // 2, PROMPT + 1), jax.random.fold_in(key_list[2], 1), PROMPT // 2, PROMPT).astype(jnp.int32)
    cotangent = scatter_about(key_list[3], (TOKENS, D), 1.0, 6.0, ((0, 32),))
    gain_self = jnp.clip(1.0 + 0.1 * jax.random.normal(key_list[4], (D,), jnp.float32), 0.5, 1.5)
    self_query = scatter_about(key_list[5], (D, D), D ** -0.5, 0.21875, ((0, 2), (1, 4)))
    self_key = scatter_about(key_list[6], (D, D), D ** -0.5, 0.21875, ((0, 2), (1, 4)))
    self_value = scatter_about(key_list[7], (D, D), D ** -0.5, 0.21875, ((0, 2), (1, 4)))
    self_out = scatter_about(key_list[8], (D, D), 4 ** -0.5, 3.0, ((0, 4), (1, 2)))
    gain_cross = jnp.clip(1.0 + 0.1 * jax.random.normal(key_list[9], (D,), jnp.float32), 0.5, 1.5)
    cross_query = scatter_about(key_list[10], (D, D), D ** -0.5, 0.21875, ((0, 2), (1, 4)))
    cross_key = scatter_about(key_list[11], (D, D), D ** -0.5, 0.21875, ((0, 2), (1, 4)))
    cross_value = scatter_about(key_list[12], (D, D), D ** -0.5, 0.21875, ((0, 2), (1, 4)))
    cross_out = scatter_about(key_list[13], (D, D), 2 ** -0.5, 4.0, ((0, 4), (1, 2)))
    gain_hidden = jnp.clip(1.0 + 0.1 * jax.random.normal(key_list[14], (D,), jnp.float32), 0.5, 1.5)
    hidden_up = scatter_about(key_list[15], (D, FF), D ** -0.5, 0.21875, ((0, 2), (1, 4)))
    hidden_down = scatter_about(key_list[16], (FF, D), FF ** -0.5, 0.109375, ((0, 4), (1, 2)))
    gain_final = jnp.clip(1.0 + 0.1 * jax.random.normal(key_list[17], (D,), jnp.float32), 0.5, 1.5)
    return {"tokens": tokens, "encoded": encoded, "branch": branch, "cotangent": cotangent, "gain_self": gain_self, "self_query": self_query, "self_key": self_key, "self_value": self_value, "self_out": self_out, "gain_cross": gain_cross, "cross_query": cross_query, "cross_key": cross_key, "cross_value": cross_value, "cross_out": cross_out, "gain_hidden": gain_hidden, "hidden_up": hidden_up, "hidden_down": hidden_down, "gain_final": gain_final}


@jax.custom_vjp
def low(v):
    return lax.optimization_barrier(v.astype(jnp.bfloat16)).astype(jnp.float32)

@jax.custom_vjp
def low_back(v):
    return v

def low_keep(v):
    return (low(v), None)

def low_pass(kept, grad):
    return (grad,)

def back_keep(v):
    return (v, None)

def back_low(kept, grad):
    return (low(grad),)
low.defvjp(low_keep, low_pass)
low_back.defvjp(back_keep, back_low)
eps = 1e-05
big_neg = -1e+30
highest = lax.Precision.HIGHEST

def product(left, right):
    return jnp.dot(left, right, precision=highest)

def normalize(rows_in, gain):
    average = lax.optimization_barrier(jnp.mean(rows_in, axis=-1, keepdims=True))
    centred = rows_in - average
    variance = lax.optimization_barrier(jnp.mean(centred * centred, axis=-1, keepdims=True))
    return centred * lax.rsqrt(variance + eps) * gain

def visible(query_pos, key_pos, branch_row):
    query_at = query_pos[:, None]
    key_at = key_pos[None, :]
    query_cont = (query_at - PROMPT) // CONT
    key_cont = (key_at - PROMPT) // CONT
    chosen = (query_cont == jnp.arange(NCONT, dtype=jnp.int32)[None, :]).astype(jnp.int32)
    limit = lax.optimization_barrier(jnp.sum(chosen * branch_row[None, :], axis=1, keepdims=True))
    same_cont = (key_cont == query_cont) & (key_at <= query_at)
    return jnp.where(query_at < PROMPT, key_at <= query_at, jnp.where(key_at < PROMPT, key_at < limit, same_cont))

def attention(queries, key_rows, value_rows, branch_row):
    length = queries.shape[0]
    block_rows = min(512, length)
    blocks = length // block_rows
    head_count = queries.shape[1] // HEAD_DIM
    scaling = HEAD_DIM ** (-0.5)
    split_q = queries.reshape(blocks, block_rows, head_count, HEAD_DIM)
    split_k = key_rows.reshape(key_rows.shape[0], head_count, HEAD_DIM)
    split_v = value_rows.reshape(value_rows.shape[0], head_count, HEAD_DIM)
    key_pos = jnp.arange(key_rows.shape[0], dtype=jnp.int32)

    @jax.checkpoint
    def one_block(inputs):
        piece, anchor = inputs
        scores = low_back(jnp.einsum('qhd,khd->hqk', piece, split_k, precision=highest) * scaling)
        if branch_row is not None:
            shown = visible(anchor + jnp.arange(block_rows, dtype=jnp.int32), key_pos, branch_row)
            scores = jnp.where(shown[None], scores, big_neg)
        weights = low(jax.nn.softmax(scores, axis=-1))
        blended = jnp.einsum('hqk,khd->qhd', weights, split_v, precision=highest)
        return blended.reshape(block_rows, head_count * HEAD_DIM)
    starts = jnp.arange(blocks, dtype=jnp.int32) * block_rows
    return lax.map(one_block, (split_q, starts)).reshape(length, head_count * HEAD_DIM)

def decoder_layer(tokens, encoded, gain_self, self_query, self_key, self_value, self_out, gain_cross, cross_query, cross_key, cross_value, cross_out, gain_hidden, hidden_up, hidden_down, gain_final, branch):
    families = branch.shape[0]
    family_shape = (families, FAMLEN, D)
    frame_shape = (families, FRAMES, D)
    normed = low(normalize(tokens, gain_self))
    queries = low_back(low(product(normed, self_query)))
    key_rows = low_back(low(product(normed, self_key)))
    value_rows = low_back(low(product(normed, self_value)))

    def self_family(inputs):
        return attention(inputs[0], inputs[1], inputs[2], inputs[3])
    blended = lax.map(jax.checkpoint(self_family), (queries.reshape(family_shape), key_rows.reshape(family_shape), value_rows.reshape(family_shape), branch))
    blended = low_back(low(blended.reshape(-1, D)))
    after_self = tokens + low_back(product(blended, self_out))
    normed = low(normalize(after_self, gain_cross))
    queries = low_back(low(product(normed, cross_query)))
    key_rows = low_back(low(product(encoded, cross_key)))
    value_rows = low_back(low(product(encoded, cross_value)))

    def cross_family(inputs):
        return attention(inputs[0], inputs[1], inputs[2], None)
    blended = lax.map(jax.checkpoint(cross_family), (queries.reshape(family_shape), key_rows.reshape(frame_shape), value_rows.reshape(frame_shape)))
    blended = low_back(low(blended.reshape(-1, D)))
    after_cross = after_self + low_back(product(blended, cross_out))
    normed = low(normalize(after_cross, gain_hidden))
    raised = low_back(product(normed, hidden_up))
    active = low(jax.nn.gelu(raised, approximate=False))
    after_hidden = after_cross + low_back(product(active, hidden_down))
    return normalize(after_hidden, gain_final)

def reference(tokens, encoded, branch, cotangent, gain_self, self_query, self_key, self_value, self_out, gain_cross, cross_query, cross_key, cross_value, cross_out, gain_hidden, hidden_up, hidden_down, gain_final):
    floats = tuple((argument.astype(jnp.float32) for argument in (tokens, encoded, gain_self, self_query, self_key, self_value, self_out, gain_cross, cross_query, cross_key, cross_value, cross_out, gain_hidden, hidden_up, hidden_down, gain_final)))

    def forward(*inputs):
        return decoder_layer(*inputs, branch)
    output, pullback = jax.vjp(forward, *floats)
    grads = pullback(cotangent.astype(jnp.float32))
    return (output.astype(jnp.bfloat16), grads[0], grads[1], grads[2], grads[3], grads[4], grads[5], grads[6], grads[7], grads[8], grads[9], grads[10], grads[11], grads[12], grads[13], grads[14], grads[15])
```

```python
import functools

import jax
import jax.numpy as jnp
from jax import lax
from jax.experimental import pallas as pl
from jax.experimental.pallas import tpu as pltpu
from jax.sharding import PartitionSpec as P

HEAD_DIM = 64
PROMPT = 1024
CONT = 256
NCONT = 4
PAIR = 2 * HEAD_DIM
LOG2E = 1.4426950408889634

eps = 1e-05
big_neg = -1e30
bf16 = jnp.bfloat16
f32 = jnp.float32


def dot(left, right, contract, dtype=f32):
    out = lax.dot_general(left, right, (contract, ((), ())), preferred_element_type=f32)
    return out.astype(dtype)


def nn(left, right, dtype=f32):
    return dot(left, right, ((1,), (0,)), dtype)


def nt(left, right, dtype=f32):
    return dot(left, right, ((1,), (1,)), dtype)


def tn(left, right, dtype=f32):
    return dot(left, right, ((0,), (0,)), dtype)


def unit_rows(rows_in):
    average = jnp.mean(rows_in, axis=-1, keepdims=True)
    centred = rows_in - average
    variance = jnp.mean(centred * centred, axis=-1, keepdims=True)
    scale = lax.rsqrt(variance + eps)
    return centred * scale, scale


def norm_back(unit, scale, gain, upstream):
    cw = upstream * gain
    first = jnp.mean(cw, axis=-1, keepdims=True)
    second = jnp.mean(cw * unit, axis=-1, keepdims=True)
    return scale * (cw - first - unit * second)


def head_masks(rows):
    lane = lax.broadcasted_iota(jnp.int32, (rows, PAIR), 1)
    return (lane < HEAD_DIM, lane >= HEAD_DIM)


def masked_scores(q, keys, limits):
    out = []
    for k, limit in zip(keys, limits):
        s = nt(q, k) * LOG2E
        if limit is not None:
            where, bound = limit
            s = jnp.where(where < bound, s, big_neg)
        out.append(s)
    return out


def fwd_body(q_ref, kv_refs, limits, o_ref, lse_ref):
    rows = q_ref.shape[0]
    masks = head_masks(rows)
    q = q_ref[...] * jnp.asarray(HEAD_DIM**-0.5, bf16)
    keys = [k[...] for k, _ in kv_refs]
    values = [v[...] for _, v in kv_refs]
    blended, logs = [], []
    for mask in masks:
        scores = masked_scores(jnp.where(mask, q, 0), keys, limits)
        top = functools.reduce(
            jnp.maximum, [jnp.max(s, axis=-1, keepdims=True) for s in scores]
        )
        raised = [jnp.exp2(s - top) for s in scores]
        total = functools.reduce(
            jnp.add, [jnp.sum(p, axis=-1, keepdims=True) for p in raised]
        )
        mixed = functools.reduce(
            jnp.add, [nn(p.astype(bf16), v) for p, v in zip(raised, values)]
        )
        blended.append(mixed / total)
        logs.append(top + jnp.log2(total))
    o_ref[...] = jnp.where(masks[0], blended[0], blended[1]).astype(bf16)
    lse_ref[...] = jnp.where(masks[0], logs[0], logs[1])


def bwd_body(q_ref, do_ref, o_ref, lse_ref, kv_refs, limits, dq_ref):
    rows = q_ref.shape[0]
    masks = head_masks(rows)
    q = q_ref[...] * jnp.asarray(HEAD_DIM**-0.5, bf16)
    grad = do_ref[...]
    product = grad.astype(f32) * o_ref[...].astype(f32)
    lse = lse_ref[...]
    keys = [k[...] for k, _ in kv_refs]
    values = [v[...] for _, v in kv_refs]
    sums_k = [None] * len(keys)
    sums_v = [None] * len(keys)
    grads_q = []
    for h, mask in enumerate(masks):
        qh = jnp.where(mask, q, 0)
        gh = jnp.where(mask, grad, 0)
        delta = jnp.sum(jnp.where(mask, product, 0), axis=-1, keepdims=True)
        level = lse[:, h * HEAD_DIM : h * HEAD_DIM + 1]
        scores = masked_scores(qh, keys, limits)
        grad_q = None
        for i, s in enumerate(scores):
            p = jnp.exp2(s - level)
            through = nt(gh, values[i])
            slope = (p * (through - delta)).astype(bf16)
            part = nn(slope, keys[i])
            grad_q = part if grad_q is None else grad_q + part
            dk, dv = tn(qh, slope), tn(gh, p.astype(bf16))
            sums_k[i] = dk if sums_k[i] is None else sums_k[i] + dk
            sums_v[i] = dv if sums_v[i] is None else sums_v[i] + dv
        grads_q.append(grad_q)
    mixed = jnp.where(masks[0], grads_q[0], grads_q[1]) * HEAD_DIM**-0.5
    dq_ref[...] = mixed.astype(bf16)
    return sums_k, sums_v


def cross_limits(width, frames):
    return lambda shape: (lax.broadcasted_iota(jnp.int32, shape, 1) % width, frames)


def self_fwd_kernel(q_ref, kc_ref, vc_ref, ko_ref, vo_ref, at_ref, lim_ref, o_ref, lse_ref):
    lim = lim_ref[...]
    own = lax.broadcasted_iota(jnp.int32, (1, ko_ref.shape[0]), 1)
    limits = [(at_ref[...], lim[:, 0:1]), (own, lim[:, 1:2])]
    fwd_body(q_ref, [(kc_ref, vc_ref), (ko_ref, vo_ref)], limits, o_ref, lse_ref)


def cross_fwd_kernel(q_ref, k_ref, v_ref, at_ref, o_ref, lse_ref, *, frames):
    limits = [(at_ref[...], frames)]
    fwd_body(q_ref, [(k_ref, v_ref)], limits, o_ref, lse_ref)


def self_bwd_kernel(
    q_ref, do_ref, o_ref, lse_ref, kc_ref, vc_ref, ko_ref, vo_ref, at_ref, lim_ref,
    dq_ref, dk_ref, dv_ref, dk_acc, dv_acc,
):
    step = pl.program_id(1)
    last = pl.num_programs(1) - 1
    ctx = kc_ref.shape[0]
    block = ko_ref.shape[0]
    lim = lim_ref[...]
    own = lax.broadcasted_iota(jnp.int32, (1, block), 1)
    limits = [(at_ref[...], lim[:, 0:1]), (own, lim[:, 1:2])]
    sums_k, sums_v = bwd_body(
        q_ref, do_ref, o_ref, lse_ref, [(kc_ref, vc_ref), (ko_ref, vo_ref)], limits, dq_ref
    )
    at = pl.multiple_of(ctx + step * block, block)
    dk_ref[pl.ds(at, block), :] = sums_k[1].T.astype(bf16)
    dv_ref[pl.ds(at, block), :] = sums_v[1].T.astype(bf16)

    @pl.when(step == 0)
    def _():
        dk_acc[...] = sums_k[0]
        dv_acc[...] = sums_v[0]

    @pl.when(step > 0)
    def _():
        dk_acc[...] += sums_k[0]
        dv_acc[...] += sums_v[0]

    @pl.when(step == last)
    def _():
        dk_ref[0:ctx, :] = dk_acc[...].T.astype(bf16)
        dv_ref[0:ctx, :] = dv_acc[...].T.astype(bf16)


def cross_bwd_kernel(
    q_ref, do_ref, o_ref, lse_ref, k_ref, v_ref, at_ref,
    dq_ref, dk_ref, dv_ref, dk_acc, dv_acc, *, frames,
):
    step = pl.program_id(1)
    last = pl.num_programs(1) - 1
    sums_k, sums_v = bwd_body(
        q_ref, do_ref, o_ref, lse_ref, [(k_ref, v_ref)], [(at_ref[...], frames)], dq_ref
    )

    @pl.when(step == 0)
    def _():
        dk_acc[...] = sums_k[0]
        dv_acc[...] = sums_v[0]

    @pl.when(step > 0)
    def _():
        dk_acc[...] += sums_k[0]
        dv_acc[...] += sums_v[0]

    @pl.when(step == last)
    def _():
        dk_ref[...] = dk_acc[...].T.astype(bf16)
        dv_ref[...] = dv_acc[...].T.astype(bf16)


def params():
    return pltpu.CompilerParams(
        dimension_semantics=("arbitrary", "arbitrary"), vmem_limit_bytes=56 * 2**20
    )


def cost(rows, keys, width, matmuls):
    return pl.CostEstimate(
        flops=2 * matmuls * rows * keys * width * 4,
        transcendentals=rows * keys * width // HEAD_DIM,
        bytes_accessed=2 * width * (4 * rows + 4 * keys),
    )


def q_spec(block):
    return pl.BlockSpec((block, PAIR), lambda p, b: (b, p))


def self_attention(q, kv, at, lim):
    rows, width = q.shape
    pairs = width // PAIR
    ctx = kv.shape[0] - rows
    first = ctx // CONT
    kinds = [
        q_spec(CONT),
        pl.BlockSpec((ctx, PAIR), lambda p, b: (0, p)),
        pl.BlockSpec((ctx, PAIR), lambda p, b: (0, pairs + p)),
        pl.BlockSpec((CONT, PAIR), lambda p, b: (first + b, p)),
        pl.BlockSpec((CONT, PAIR), lambda p, b: (first + b, pairs + p)),
        pl.BlockSpec((1, ctx), lambda p, b: (0, 0)),
        pl.BlockSpec((CONT, 2), lambda p, b: (b, 0)),
    ]
    return pl.pallas_call(
        self_fwd_kernel,
        grid=(pairs, rows // CONT),
        in_specs=kinds,
        out_specs=[q_spec(CONT), q_spec(CONT)],
        out_shape=[
            jax.ShapeDtypeStruct((rows, width), bf16),
            jax.ShapeDtypeStruct((rows, width), f32),
        ],
        compiler_params=params(),
        cost_estimate=cost(rows, ctx + CONT, width, 2),
        name="self_fwd",
    )(q, kv, kv, kv, kv, at, lim)


def self_attention_back(q, do, o, lse, kv, at, lim):
    rows, width = q.shape
    pairs = width // PAIR
    ctx = kv.shape[0] - rows
    first = ctx // CONT
    kinds = [
        q_spec(CONT), q_spec(CONT), q_spec(CONT), q_spec(CONT),
        pl.BlockSpec((ctx, PAIR), lambda p, b: (0, p)),
        pl.BlockSpec((ctx, PAIR), lambda p, b: (0, pairs + p)),
        pl.BlockSpec((CONT, PAIR), lambda p, b: (first + b, p)),
        pl.BlockSpec((CONT, PAIR), lambda p, b: (first + b, pairs + p)),
        pl.BlockSpec((1, ctx), lambda p, b: (0, 0)),
        pl.BlockSpec((CONT, 2), lambda p, b: (b, 0)),
    ]
    whole = pl.BlockSpec((ctx + rows, PAIR), lambda p, b: (0, p))
    return pl.pallas_call(
        self_bwd_kernel,
        grid=(pairs, rows // CONT),
        in_specs=kinds,
        out_specs=[q_spec(CONT), whole, whole],
        out_shape=[
            jax.ShapeDtypeStruct((rows, width), bf16),
            jax.ShapeDtypeStruct((ctx + rows, width), bf16),
            jax.ShapeDtypeStruct((ctx + rows, width), bf16),
        ],
        scratch_shapes=[pltpu.VMEM((PAIR, ctx), f32), pltpu.VMEM((PAIR, ctx), f32)],
        compiler_params=params(),
        cost_estimate=cost(rows, ctx + CONT, width, 5),
        name="self_bwd",
    )(q, do, o, lse, kv, kv, kv, kv, at, lim)


def cross_attention(q, kv, at, frames):
    rows, width = q.shape
    pairs = width // PAIR
    keys = kv.shape[0]
    return pl.pallas_call(
        functools.partial(cross_fwd_kernel, frames=frames),
        grid=(pairs, rows // CONT),
        in_specs=[
            q_spec(CONT),
            pl.BlockSpec((keys, PAIR), lambda p, b: (0, p)),
            pl.BlockSpec((keys, PAIR), lambda p, b: (0, pairs + p)),
            pl.BlockSpec((1, keys), lambda p, b: (0, 0)),
        ],
        out_specs=[q_spec(CONT), q_spec(CONT)],
        out_shape=[
            jax.ShapeDtypeStruct((rows, width), bf16),
            jax.ShapeDtypeStruct((rows, width), f32),
        ],
        compiler_params=params(),
        cost_estimate=cost(rows, keys, width, 2),
        name="cross_fwd",
    )(q, kv, kv, at)


def cross_attention_back(q, do, o, lse, kv, at, frames):
    rows, width = q.shape
    pairs = width // PAIR
    keys = kv.shape[0]
    whole = pl.BlockSpec((keys, PAIR), lambda p, b: (0, p))
    return pl.pallas_call(
        functools.partial(cross_bwd_kernel, frames=frames),
        grid=(pairs, rows // CONT),
        in_specs=[
            q_spec(CONT), q_spec(CONT), q_spec(CONT), q_spec(CONT),
            whole,
            pl.BlockSpec((keys, PAIR), lambda p, b: (0, pairs + p)),
            pl.BlockSpec((1, keys), lambda p, b: (0, 0)),
        ],
        out_specs=[q_spec(CONT), whole, whole],
        out_shape=[
            jax.ShapeDtypeStruct((rows, width), bf16),
            jax.ShapeDtypeStruct((keys, width), bf16),
            jax.ShapeDtypeStruct((keys, width), bf16),
        ],
        scratch_shapes=[pltpu.VMEM((PAIR, keys), f32), pltpu.VMEM((PAIR, keys), f32)],
        compiler_params=params(),
        cost_estimate=cost(rows, keys, width, 5),
        name="cross_bwd",
    )(q, do, o, lse, kv, kv, at)


def flip(value, axis, bit):
    size = lax.axis_size(axis)
    return lax.ppermute(value, axis, [(i, i ^ bit) for i in range(size)])


def bits(axis):
    size = lax.axis_size(axis)
    return [1 << b for b in range(size.bit_length() - 1)]


def settle(value):
    return lax.optimization_barrier(value)


def gather_blocks(shard):
    near = [[shard], [flip(shard, "row", 2)]]
    for bit in bits("col"):
        near = [list(p) + [flip(block, "col", bit) for block in p] for p in near]
    far = [[flip(block, "row", 1) for block in p] for p in near]
    return near + far


def col_order(parts):
    count = len(parts)
    place = lax.axis_index("col")
    if count == 1:
        return parts
    if count == 2:
        even = place == 0
        return [jnp.where(even, parts[0], parts[1]), jnp.where(even, parts[1], parts[0])]
    stacked = jnp.stack(parts)
    return [stacked[jnp.bitwise_xor(place, a)] for a in range(count)]


def assemble(blocks, start, stop):
    return jnp.concatenate(
        [
            jnp.concatenate(col_order([b[start:stop] for b in piece]), axis=1)
            for piece in blocks
        ],
        axis=0,
    )


def col_halves(value):
    count = lax.axis_size("col")
    width = value.shape[1] // count
    return [value[:, i * width : (i + 1) * width] for i in range(count)]


def reduce_weights(grads):
    kept = []
    for g in grads:
        half = g.shape[0] // 2
        got = flip(g[half:], "row", 1)
        kept.append((g[:half].astype(f32) + got.astype(f32)).astype(bf16))
    sizes = [k.shape[0] // 2 for k in kept]
    joined = jnp.concatenate([k[:s] for k, s in zip(kept, sizes)] + [k[s:] for k, s in zip(kept, sizes)])
    parts = col_order(col_halves(joined))
    for bit in reversed(bits("col")):
        keep, send = parts[:bit], parts[bit:]
        got = [flip(s, "col", bit) for s in send]
        parts = [(a.astype(f32) + b.astype(f32)).astype(bf16) for a, b in zip(keep, got)]
    total = parts[0]
    half = total.shape[0] // 2
    got = flip(total[half:], "row", 2)
    total = settle((total[:half].astype(f32) + got.astype(f32)).astype(bf16))
    for bit in bits("dp")[:-1]:
        got = flip(total, "dp", bit)
        total = settle((total.astype(f32) + got.astype(f32)).astype(bf16))
    got = flip(total, "dp", bits("dp")[-1])
    total = total.astype(f32) + got.astype(f32)
    out, at = [], 0
    for s in sizes:
        out.append(total[at : at + s])
        at += s
    return out


def sum_all(value):
    for axis in ("row", "col", "dp"):
        for bit in bits(axis):
            value = value + flip(value, axis, bit)
    return value


def local(
    tokens,
    encoded,
    branch,
    cotangent,
    gain_self,
    self_query,
    self_key,
    self_value,
    self_out,
    gain_cross,
    cross_query,
    cross_key,
    cross_value,
    cross_out,
    gain_hidden,
    hidden_up,
    hidden_down,
    gain_final,
):
    row = lax.axis_index("row")
    rows, width = tokens.shape
    frames = encoded.shape[0]
    padded = -(-frames // 128) * 128
    r = self_query.shape[1]
    rf = hidden_up.shape[1]

    group_a = jnp.concatenate([self_query.T, self_key.T, self_value.T])
    group_b = jnp.concatenate([self_out, cross_query.T, cross_key.T, cross_value.T, cross_out])
    group_c = jnp.concatenate([hidden_up.T, hidden_down])
    blocks_a = gather_blocks(group_a)
    moved = lax.ppermute(tokens, "row", [(0, 2), (1, 3)])
    slot = jnp.where(row < 2, tokens, moved)
    context = jnp.concatenate([slot, flip(slot, "row", 1)])
    piece = jnp.pad(encoded, ((0, padded - frames), (0, 0)))
    near = jnp.concatenate([piece, flip(piece, "row", 2)])
    e = jnp.concatenate([near, flip(near, "row", 1)])
    blocks_b = gather_blocks(group_b)
    blocks_c = gather_blocks(group_c)

    position = row * rows + jnp.arange(rows, dtype=jnp.int32)
    chosen = (position - PROMPT) // CONT
    chosen = (chosen[:, None] == jnp.arange(NCONT, dtype=jnp.int32)[None, :]).astype(jnp.int32)
    cut = jnp.sum(chosen * branch[0][None, :], axis=1)
    is_prompt = position < PROMPT
    lim = jnp.stack(
        [
            jnp.where(is_prompt, position + 1, cut),
            jnp.where(is_prompt, 0, position % CONT + 1),
        ],
        axis=1,
    )
    offsets = jnp.arange(rows, dtype=jnp.int32)
    side = jnp.bitwise_and(row, 1)
    at_self = jnp.concatenate([side * rows + offsets, (1 - side) * rows + offsets])[None, :]
    at_cross = (jnp.arange(4 * padded, dtype=jnp.int32) % padded)[None, :]

    w_q = assemble(blocks_a, 0, r)
    w_k = assemble(blocks_a, r, 2 * r)
    w_v = assemble(blocks_a, 2 * r, 3 * r)
    w_kv = jnp.concatenate([w_k, w_v])
    x = tokens.astype(f32)
    n1, z1 = unit_rows(x)
    a1 = (n1 * gain_self).astype(bf16)
    a1_context = (unit_rows(context.astype(f32))[0] * gain_self).astype(bf16)
    a1_all = jnp.concatenate([a1_context, a1])
    q = nt(a1, w_q, bf16)
    kv = nt(a1_all, w_kv, bf16)
    o, lse = self_attention(q, kv, at_self, lim)
    w_o = assemble(blocks_b, 0, r)
    h1 = x + nn(o, w_o)

    w_cq = assemble(blocks_b, r, 2 * r)
    w_ck = assemble(blocks_b, 2 * r, 3 * r)
    w_cv = assemble(blocks_b, 3 * r, 4 * r)
    w_ckv = jnp.concatenate([w_ck, w_cv])
    w_co = assemble(blocks_b, 4 * r, 5 * r)
    n2, z2 = unit_rows(h1)
    a2 = (n2 * gain_cross).astype(bf16)
    cq = nt(a2, w_cq, bf16)
    ckv = nt(e, w_ckv, bf16)
    oc, lse_c = cross_attention(cq, ckv, at_cross, frames)
    h2 = h1 + nn(oc, w_co)

    w_up = assemble(blocks_c, 0, rf)
    w_down = assemble(blocks_c, rf, 2 * rf)
    n3, z3 = unit_rows(h2)
    a3 = (n3 * gain_hidden).astype(bf16)
    u = nt(a3, w_up)
    g = jax.nn.gelu(u, approximate=False).astype(bf16)
    h3 = h2 + nn(g, w_down)
    n4, z4 = unit_rows(h3)
    layer_out = (n4 * gain_final).astype(bf16)

    c3 = cotangent.astype(f32)
    gain_4 = jnp.sum(c3 * n4, axis=0)
    dh3 = norm_back(n4, z4, gain_final, c3)
    db3 = dh3.astype(bf16)
    g_down = tn(g, db3, bf16)
    _, gelu_pull = jax.vjp(lambda t: jax.nn.gelu(t, approximate=False), u)
    du = gelu_pull(nt(db3, w_down))[0].astype(bf16)
    g_up = tn(du, a3, bf16)
    (s_up, s_down) = reduce_weights([g_up, g_down])
    da3 = nn(du, w_up)
    gain_3 = jnp.sum(da3 * n3, axis=0)
    dh2 = dh3 + norm_back(n3, z3, gain_hidden, da3)
    db2 = dh2.astype(bf16)

    g_co = tn(oc, db2, bf16)
    doc = nt(db2, w_co, bf16)
    dcq, dck, dcv = cross_attention_back(cq, doc, oc, lse_c, ckv, at_cross, frames)
    g_cq = tn(dcq, a2, bf16)
    g_ck = tn(dck, e, bf16)
    g_cv = tn(dcv, e, bf16)
    de = (nn(dck, w_ck) + nn(dcv, w_cv)).astype(bf16)
    two = 2 * padded
    de = (de[:two].astype(f32) + flip(de[two:], "row", 1).astype(f32)).astype(bf16)
    grad_encoded = de[:padded].astype(f32) + flip(de[padded:], "row", 2).astype(f32)
    grad_encoded = grad_encoded[:frames]
    da2 = nn(dcq, w_cq)
    gain_2 = jnp.sum(da2 * n2, axis=0)
    dh1 = dh2 + norm_back(n2, z2, gain_cross, da2)
    db1 = dh1.astype(bf16)

    g_o = tn(o, db1, bf16)
    s_o, s_cq, s_ck, s_cv, s_co = reduce_weights([g_o, g_cq, g_ck, g_cv, g_co])
    do = nt(db1, w_o, bf16)
    dq, dk, dv = self_attention_back(q, do, o, lse, kv, at_self, lim)
    da_all = nn(dk, w_k) + nn(dv, w_v)
    ctx = PROMPT
    own = da_all[ctx:]
    mine = da_all[: ctx // 2]
    theirs = da_all[ctx // 2 : ctx].astype(bf16)
    mine = mine + flip(theirs, "row", 1).astype(f32)
    back = lax.ppermute(mine.astype(bf16), "row", [(2, 0), (3, 1)]).astype(f32)
    g_q = tn(dq, a1, bf16)
    g_k = tn(dk, a1_all, bf16)
    g_v = tn(dv, a1_all, bf16)
    s_q, s_k, s_v = reduce_weights([g_q, g_k, g_v])
    da1 = nn(dq, w_q) + own + jnp.where(row < 2, mine + back, 0.0)
    gain_1 = jnp.sum(da1 * n1, axis=0)
    grad_tokens = dh1 + norm_back(n1, z1, gain_self, da1)

    gains = sum_all(jnp.stack([gain_1, gain_2, gain_3, gain_4]))
    return (
        layer_out,
        grad_tokens,
        grad_encoded,
        gains[0],
        s_q.T,
        s_k.T,
        s_v.T,
        s_o,
        gains[1],
        s_cq.T,
        s_ck.T,
        s_cv.T,
        s_co,
        gains[2],
        s_up.T,
        s_down,
        gains[3],
    )


def solution(mesh):
    rows = P(("dp", "col", "row"), None)
    down, across = P("col", "row"), P("row", "col")
    return jax.shard_map(
        local,
        mesh=mesh,
        in_specs=(
            rows, rows, P(("dp", "col"), None), rows,
            P(), down, down, down, across,
            P(), down, down, down, across,
            P(), down, across, P(),
        ),
        out_specs=(
            rows, rows, rows,
            P(), down, down, down, across,
            P(), down, down, down, across,
            P(), down, across, P(),
        ),
        check_vma=False,
    )
```

```python
import functools

import jax
import jax.numpy as jnp
from jax import lax
from jax.experimental import pallas as pl
from jax.experimental.pallas import tpu as pltpu
from jax.sharding import PartitionSpec as P


HEAD_DIM = 64
PROMPT = 1024
CONT = 256
NCONT = 4
PAIR = 2 * HEAD_DIM
LOG2E = 1.4426950408889634

eps = 1e-05
big_neg = -1e30
bf16 = jnp.bfloat16
f32 = jnp.float32


def dot(left, right, contract, dtype=f32):
    out = lax.dot_general(left, right, (contract, ((), ())), preferred_element_type=f32)
    return out.astype(dtype)


def nn(left, right, dtype=f32):
    return dot(left, right, ((1,), (0,)), dtype)


def nt(left, right, dtype=f32):
    return dot(left, right, ((1,), (1,)), dtype)


def tn(left, right, dtype=f32):
    return dot(left, right, ((0,), (0,)), dtype)


def unit_rows(rows_in):
    average = jnp.mean(rows_in, axis=-1, keepdims=True)
    centred = rows_in - average
    variance = jnp.mean(centred * centred, axis=-1, keepdims=True)
    scale = lax.rsqrt(variance + eps)
    return centred * scale, scale


def norm_back(unit, scale, gain, upstream):
    cw = upstream * gain
    first = jnp.mean(cw, axis=-1, keepdims=True)
    second = jnp.mean(cw * unit, axis=-1, keepdims=True)
    return scale * (cw - first - unit * second)


def head_masks(rows):
    lane = lax.broadcasted_iota(jnp.int32, (rows, PAIR), 1)
    return (lane < HEAD_DIM, lane >= HEAD_DIM)


def masked_scores(q, keys, limits):
    out = []
    for k, limit in zip(keys, limits):
        s = nt(q, k) * LOG2E
        if limit is not None:
            where, bound = limit
            s = jnp.where(where < bound, s, big_neg)
        out.append(s)
    return out


def fwd_body(q_ref, kv_refs, limits, o_ref, lse_ref):
    rows = q_ref.shape[0]
    masks = head_masks(rows)
    q = q_ref[...] * jnp.asarray(HEAD_DIM**-0.5, bf16)
    keys = [k[...] for k, _ in kv_refs]
    values = [v[...] for _, v in kv_refs]
    blended, logs = [], []
    for mask in masks:
        scores = masked_scores(jnp.where(mask, q, 0), keys, limits)
        top = functools.reduce(
            jnp.maximum, [jnp.max(s, axis=-1, keepdims=True) for s in scores]
        )
        raised = [jnp.exp2(s - top) for s in scores]
        total = functools.reduce(
            jnp.add, [jnp.sum(p, axis=-1, keepdims=True) for p in raised]
        )
        mixed = functools.reduce(
            jnp.add, [nn(p.astype(bf16), v) for p, v in zip(raised, values)]
        )
        blended.append(mixed / total)
        logs.append(top + jnp.log2(total))
    o_ref[...] = jnp.where(masks[0], blended[0], blended[1]).astype(bf16)
    lse_ref[...] = jnp.where(masks[0], logs[0], logs[1])


def bwd_body(q_ref, do_ref, o_ref, lse_ref, kv_refs, limits, dq_ref):
    rows = q_ref.shape[0]
    masks = head_masks(rows)
    q = q_ref[...] * jnp.asarray(HEAD_DIM**-0.5, bf16)
    grad = do_ref[...]
    product = grad.astype(f32) * o_ref[...].astype(f32)
    lse = lse_ref[...]
    keys = [k[...] for k, _ in kv_refs]
    values = [v[...] for _, v in kv_refs]
    sums_k = [None] * len(keys)
    sums_v = [None] * len(keys)
    grads_q = []
    for h, mask in enumerate(masks):
        qh = jnp.where(mask, q, 0)
        gh = jnp.where(mask, grad, 0)
        delta = jnp.sum(jnp.where(mask, product, 0), axis=-1, keepdims=True)
        level = lse[:, h * HEAD_DIM : h * HEAD_DIM + 1]
        scores = masked_scores(qh, keys, limits)
        grad_q = None
        for i, s in enumerate(scores):
            p = jnp.exp2(s - level)
            through = nt(gh, values[i])
            slope = (p * (through - delta)).astype(bf16)
            part = nn(slope, keys[i])
            grad_q = part if grad_q is None else grad_q + part
            dk, dv = tn(qh, slope), tn(gh, p.astype(bf16))
            sums_k[i] = dk if sums_k[i] is None else sums_k[i] + dk
            sums_v[i] = dv if sums_v[i] is None else sums_v[i] + dv
        grads_q.append(grad_q)
    mixed = jnp.where(masks[0], grads_q[0], grads_q[1]) * HEAD_DIM**-0.5
    dq_ref[...] = mixed.astype(bf16)
    return sums_k, sums_v


def self_fwd_kernel(q_ref, kc_ref, vc_ref, ko_ref, vo_ref, at_ref, lim_ref, o_ref, lse_ref):
    lim = lim_ref[...]
    own = lax.broadcasted_iota(jnp.int32, (1, ko_ref.shape[0]), 1)
    limits = [(at_ref[...], lim[:, 0:1]), (own, lim[:, 1:2])]
    fwd_body(q_ref, [(kc_ref, vc_ref), (ko_ref, vo_ref)], limits, o_ref, lse_ref)


def cross_fwd_kernel(q_ref, k_ref, v_ref, at_ref, o_ref, lse_ref, *, frames):
    limits = [(at_ref[...], frames)]
    fwd_body(q_ref, [(k_ref, v_ref)], limits, o_ref, lse_ref)


def self_bwd_kernel(
    q_ref, do_ref, o_ref, lse_ref, kc_ref, vc_ref, ko_ref, vo_ref, at_ref, lim_ref,
    dq_ref, dk_ref, dv_ref, dk_acc, dv_acc,
):
    step = pl.program_id(1)
    last = pl.num_programs(1) - 1
    ctx = kc_ref.shape[0]
    block = ko_ref.shape[0]
    lim = lim_ref[...]
    own = lax.broadcasted_iota(jnp.int32, (1, block), 1)
    limits = [(at_ref[...], lim[:, 0:1]), (own, lim[:, 1:2])]
    sums_k, sums_v = bwd_body(
        q_ref, do_ref, o_ref, lse_ref, [(kc_ref, vc_ref), (ko_ref, vo_ref)], limits, dq_ref
    )
    at = pl.multiple_of(ctx + step * block, block)
    dk_ref[pl.ds(at, block), :] = sums_k[1].T.astype(bf16)
    dv_ref[pl.ds(at, block), :] = sums_v[1].T.astype(bf16)

    @pl.when(step == 0)
    def _():
        dk_acc[...] = sums_k[0]
        dv_acc[...] = sums_v[0]

    @pl.when(step > 0)
    def _():
        dk_acc[...] += sums_k[0]
        dv_acc[...] += sums_v[0]

    @pl.when(step == last)
    def _():
        dk_ref[0:ctx, :] = dk_acc[...].T.astype(bf16)
        dv_ref[0:ctx, :] = dv_acc[...].T.astype(bf16)


def cross_bwd_kernel(
    q_ref, do_ref, o_ref, lse_ref, k_ref, v_ref, at_ref,
    dq_ref, dk_ref, dv_ref, dk_acc, dv_acc, *, frames,
):
    step = pl.program_id(1)
    last = pl.num_programs(1) - 1
    sums_k, sums_v = bwd_body(
        q_ref, do_ref, o_ref, lse_ref, [(k_ref, v_ref)], [(at_ref[...], frames)], dq_ref
    )

    @pl.when(step == 0)
    def _():
        dk_acc[...] = sums_k[0]
        dv_acc[...] = sums_v[0]

    @pl.when(step > 0)
    def _():
        dk_acc[...] += sums_k[0]
        dv_acc[...] += sums_v[0]

    @pl.when(step == last)
    def _():
        dk_ref[...] = dk_acc[...].T.astype(bf16)
        dv_ref[...] = dv_acc[...].T.astype(bf16)


def params():
    return pltpu.CompilerParams(
        dimension_semantics=("arbitrary", "arbitrary"), vmem_limit_bytes=56 * 2**20
    )


def cost(rows, keys, width, matmuls):
    return pl.CostEstimate(
        flops=2 * matmuls * rows * keys * width * 4,
        transcendentals=rows * keys * width // HEAD_DIM,
        bytes_accessed=2 * width * (4 * rows + 4 * keys),
    )


def in_parts(kernel, parts, width, ins, specs, out_specs, shapes, scratch, grid_rows, estimate):
    pairs = width // PAIR
    step = pairs // parts
    outs = None
    for i in range(parts):
        first = i * step

        def moved(spec, first=first):
            if spec is None:
                return pl.BlockSpec(memory_space=pl.ANY)
            block, index = spec
            return pl.BlockSpec(block, lambda p, b: index(p + first, b))

        given = list(ins) + (list(outs) if outs else [])
        extra = len(outs) if outs else 0

        def body(*refs, extra=extra):
            kernel(*refs[: len(ins)], *refs[len(ins) + extra :])

        outs = pl.pallas_call(
            body,
            grid=(step, grid_rows),
            in_specs=[moved(spec) for spec in specs] + [moved(None)] * extra,
            out_specs=[moved(spec) for spec in out_specs],
            out_shape=shapes,
            scratch_shapes=scratch,
            input_output_aliases={len(ins) + j: j for j in range(extra)},
            compiler_params=params(),
            cost_estimate=estimate(width // parts),
        )(*given)
    return outs


def q_spec(block):
    return ((block, PAIR), lambda p, b: (b, p))


def sds(rows, width, kind):
    return jax.ShapeDtypeStruct((rows, width), kind)


def self_specs(ctx):
    first = ctx // CONT
    context = ((ctx, PAIR), lambda p, b: (0, p))
    own = ((CONT, PAIR), lambda p, b: (first + b, p))
    return [
        context, context, own, own,
        ((1, ctx), lambda p, b: (0, 0)),
        ((CONT, 2), lambda p, b: (b, 0)),
    ]


def self_attention(q, k, v, at, lim, parts):
    rows, width = q.shape
    ctx = k.shape[0] - rows
    return in_parts(
        self_fwd_kernel, parts, width,
        (q, k, v, k, v, at, lim), [q_spec(CONT)] + self_specs(ctx),
        [q_spec(CONT)] * 2, [sds(rows, width, bf16), sds(rows, width, f32)], [],
        rows // CONT, lambda w: cost(rows, ctx + CONT, w, 2),
    )


def self_attention_back(q, do, o, lse, k, v, at, lim, parts):
    rows, width = q.shape
    ctx = k.shape[0] - rows
    whole = ((ctx + rows, PAIR), lambda p, b: (0, p))
    return in_parts(
        self_bwd_kernel, parts, width,
        (q, do, o, lse, k, v, k, v, at, lim), [q_spec(CONT)] * 4 + self_specs(ctx),
        [q_spec(CONT), whole, whole],
        [sds(rows, width, bf16), sds(ctx + rows, width, bf16), sds(ctx + rows, width, bf16)],
        [pltpu.VMEM((PAIR, ctx), f32), pltpu.VMEM((PAIR, ctx), f32)],
        rows // CONT, lambda w: cost(rows, ctx + CONT, w, 5),
    )


def cross_attention(q, k, v, at, frames, parts):
    rows, width = q.shape
    keys = k.shape[0]
    whole = ((keys, PAIR), lambda p, b: (0, p))
    return in_parts(
        functools.partial(cross_fwd_kernel, frames=frames), parts, width,
        (q, k, v, at), [q_spec(CONT), whole, whole, ((1, keys), lambda p, b: (0, 0))],
        [q_spec(CONT)] * 2, [sds(rows, width, bf16), sds(rows, width, f32)], [],
        rows // CONT, lambda w: cost(rows, keys, w, 2),
    )


def cross_attention_back(q, do, o, lse, k, v, at, frames, parts):
    rows, width = q.shape
    keys = k.shape[0]
    whole = ((keys, PAIR), lambda p, b: (0, p))
    return in_parts(
        functools.partial(cross_bwd_kernel, frames=frames), parts, width,
        (q, do, o, lse, k, v, at),
        [q_spec(CONT)] * 4 + [whole, whole, ((1, keys), lambda p, b: (0, 0))],
        [q_spec(CONT), whole, whole],
        [sds(rows, width, bf16), sds(keys, width, bf16), sds(keys, width, bf16)],
        [pltpu.VMEM((PAIR, keys), f32), pltpu.VMEM((PAIR, keys), f32)],
        rows // CONT, lambda w: cost(rows, keys, w, 5),
    )


def flip(value, axis, bit):
    size = lax.axis_size(axis)
    return lax.ppermute(value, axis, [(i, i ^ bit) for i in range(size)])


def bits(axis):
    size = lax.axis_size(axis)
    return [1 << b for b in range(size.bit_length() - 1)]


def settle(value):
    return lax.optimization_barrier(value)


def pack_kernel(turned, *refs):
    out, at = refs[-1], 0
    for ref, turn in zip(refs[:-1], turned):
        value = ref[...]
        if turn:
            value = value.astype(f32).T.astype(bf16)
        out[at : at + value.shape[0], :] = value
        at += value.shape[0]


def pack(weights, turned):
    rows = sum(w.shape[1] if t else w.shape[0] for w, t in zip(weights, turned))
    width = weights[0].shape[0] if turned[0] else weights[0].shape[1]
    if width % 128:
        return jnp.concatenate([w.T if t else w for w, t in zip(weights, turned)])
    return pl.pallas_call(
        functools.partial(pack_kernel, turned),
        out_shape=sds(rows, width, bf16),
        grid=(1,),
        in_specs=[pl.BlockSpec(w.shape, lambda i: (0, 0)) for w in weights],
        out_specs=pl.BlockSpec((rows, width), lambda i: (0, 0)),
        compiler_params=pltpu.CompilerParams(vmem_limit_bytes=16 * 2**20),
        cost_estimate=pl.CostEstimate(flops=0, transcendentals=0, bytes_accessed=4 * rows * width),
        name="pack",
    )(*weights)


def col_order(parts):
    count = len(parts)
    place = lax.axis_index("col")
    if count == 1:
        return parts
    if count == 2:
        even = place == 0
        return [jnp.where(even, parts[0], parts[1]), jnp.where(even, parts[1], parts[0])]
    stacked = jnp.stack(parts)
    return [stacked[jnp.bitwise_xor(place, a)] for a in range(count)]


def near_blocks(shard):
    near = [[shard], [flip(shard, "row", 2)]]
    for bit in bits("col"):
        near = [list(p) + [flip(block, "col", bit) for block in p] for p in near]
    return near


def spread_kernel(r, count, plain, *refs):
    sources = refs[: 4 + len(plain)]
    outs = refs[4 + len(plain) : 4 + len(plain) + count + (1 if plain else 0)]
    rest = refs[4 + len(plain) + count + (1 if plain else 0) :]
    buffers, (in_sem, out_sem, send_sem, recv_sem) = rest[:-4], rest[-4:]
    width = sources[0].shape[1]
    me = lax.axis_index("row")
    partner = {"row": me + 1 - 2 * lax.rem(me, 2)}
    place = lax.axis_index("col")

    barrier = pltpu.get_barrier_semaphore()
    pl.semaphore_signal(barrier, inc=1, device_id=partner, device_id_type=pl.DeviceIdType.MESH)
    loads = []
    for i, source in enumerate(sources):
        buffer = buffers[0].at[i] if i < 4 else buffers[1].at[i - 4]
        load = pltpu.make_async_copy(source, buffer, in_sem.at[i])
        load.start()
        loads.append(load)
    pl.semaphore_wait(barrier, 1)
    waits, n = [], 0

    def place_both(piece, here, there):
        nonlocal n
        local_copy = pltpu.make_async_copy(piece, here, out_sem.at[n])
        remote_copy = pltpu.make_async_remote_copy(
            src_ref=piece, dst_ref=there, send_sem=send_sem.at[n], recv_sem=recv_sem.at[n],
            device_id=partner, device_id_type=pl.DeviceIdType.MESH,
        )
        local_copy.start()
        remote_copy.start()
        waits.append((local_copy, remote_copy))
        n += 1

    for i in range(4):
        p, j = i // 2, i % 2
        loads[i].wait()
        side = place if j == 0 else 1 - place
        lanes = pl.ds(pl.multiple_of(side * width, 128), width)
        for w in range(count):
            piece = buffers[0].at[i, pl.ds(w * r, r), :]
            place_both(
                piece,
                outs[w].at[pl.ds(p * r, r), lanes],
                outs[w].at[pl.ds((p + 2) * r, r), lanes],
            )
    for i, rows in enumerate(plain):
        loads[4 + i].wait()
        place_both(
            buffers[1].at[i],
            outs[count].at[pl.ds(i * rows, rows), :],
            outs[count].at[pl.ds((len(plain) + i) * rows, rows), :],
        )
    for local_copy, remote_copy in waits:
        local_copy.wait()
        remote_copy.wait()


def spread(blocks, r, plain, number):
    rows, width = blocks[0][0].shape
    count = rows // r
    if lax.axis_size("col") != 2 or width % 128:
        every = blocks + [[flip(b, "row", 1) for b in p] for p in blocks]
        outs = [
            jnp.concatenate(
                [
                    jnp.concatenate(col_order([b[w * r : (w + 1) * r] for b in p]), axis=1)
                    for p in every
                ]
            )
            for w in range(count)
        ]
        if plain:
            outs.append(jnp.concatenate(list(plain) + [flip(x, "row", 1) for x in plain]))
        return outs
    flat = [b for p in blocks for b in p]
    moves = 4 * count + len(plain)
    shapes = [sds(4 * r, 2 * width, bf16)] * count
    scratch = [pltpu.VMEM((4, rows, width), bf16)]
    if plain:
        n, wide = plain[0].shape
        shapes = shapes + [sds(2 * len(plain) * n, wide, bf16)]
        scratch.append(pltpu.VMEM((len(plain), n, wide), bf16))
    any_place = pl.BlockSpec(memory_space=pl.ANY)
    return pl.pallas_call(
        functools.partial(spread_kernel, r, count, tuple(x.shape[0] for x in plain)),
        out_shape=shapes,
        in_specs=[any_place] * (4 + len(plain)),
        out_specs=[any_place] * len(shapes),
        scratch_shapes=scratch
        + [
            pltpu.SemaphoreType.DMA((4 + len(plain),)),
            pltpu.SemaphoreType.DMA((moves,)),
            pltpu.SemaphoreType.DMA((moves,)),
            pltpu.SemaphoreType.DMA((moves,)),
        ],
        compiler_params=pltpu.CompilerParams(
            collective_id=number, has_side_effects=True, vmem_limit_bytes=24 * 2**20
        ),
        cost_estimate=pl.CostEstimate(flops=0, transcendentals=0, bytes_accessed=24 * rows * width),
    )(*flat, *plain)


def col_halves(value):
    count = lax.axis_size("col")
    width = value.shape[1] // count
    return [value[:, i * width : (i + 1) * width] for i in range(count)]


def add(a, b):
    return (a.astype(f32) + b.astype(f32)).astype(bf16)


def reduce_weights(grads):
    kept = []
    for g in grads:
        half = g.shape[0] // 2
        kept.append(add(g[:half], flip(g[half:], "row", 1)))
    sizes = [k.shape[0] // 2 for k in kept]
    joined = jnp.concatenate(
        [k[:s] for k, s in zip(kept, sizes)] + [k[s:] for k, s in zip(kept, sizes)]
    )
    parts = col_order(col_halves(joined))
    for bit in reversed(bits("col")):
        keep, send = parts[:bit], parts[bit:]
        parts = [add(a, flip(b, "col", bit)) for a, b in zip(keep, send)]
    total = parts[0]
    half = total.shape[0] // 2
    total = settle(add(total[:half], flip(total[half:], "row", 2)))
    for bit in bits("dp")[:-1]:
        total = settle(add(total, flip(total, "dp", bit)))
    last = bits("dp")[-1]
    total = total.astype(f32) + flip(total, "dp", last).astype(f32)
    out, at = [], 0
    for s in sizes:
        out.append(total[at : at + s])
        at += s
    return out


def sum_all(value):
    for axis, bit in [("row", 1), ("col", None), ("row", 2), ("dp", None)]:
        for b in bits(axis) if bit is None else [bit]:
            value = value + flip(value, axis, b)
    return value


def layer(
    tokens,
    encoded,
    branch,
    cotangent,
    gain_self,
    self_query,
    self_key,
    self_value,
    self_out,
    gain_cross,
    cross_query,
    cross_key,
    cross_value,
    cross_out,
    gain_hidden,
    hidden_up,
    hidden_down,
    gain_final,
):
    row = lax.axis_index("row")
    rows, _ = tokens.shape
    frames = encoded.shape[0]
    padded = -(-frames // 128) * 128
    r = self_query.shape[1]
    rf = hidden_up.shape[1]

    blocks_a = near_blocks(pack((self_query, self_key, self_value), (True, True, True)))
    moved = lax.ppermute(tokens, "row", [(0, 2), (1, 3)])
    slot = jnp.where(row < 2, tokens, moved)
    blocks_b = near_blocks(
        pack(
            (self_out, cross_query, cross_key, cross_value, cross_out),
            (False, True, True, True, False),
        ),
    )
    piece = jnp.pad(encoded, ((0, padded - frames), (0, 0)))
    other = flip(piece, "row", 2)
    blocks_c = near_blocks(pack((hidden_up,), (True,)))
    blocks_f = near_blocks(hidden_down)

    position = row * rows + jnp.arange(rows, dtype=jnp.int32)
    chosen = (position - PROMPT) // CONT
    chosen = (chosen[:, None] == jnp.arange(NCONT, dtype=jnp.int32)[None, :]).astype(jnp.int32)
    cut = jnp.sum(chosen * branch[0][None, :], axis=1)
    is_prompt = position < PROMPT
    lim = jnp.stack(
        [
            jnp.where(is_prompt, position + 1, cut),
            jnp.where(is_prompt, 0, position % CONT + 1),
        ],
        axis=1,
    )
    offsets = jnp.arange(rows, dtype=jnp.int32)
    side = jnp.bitwise_and(row, 1)
    at_self = jnp.concatenate([side * rows + offsets, (1 - side) * rows + offsets])[None, :]
    at_cross = (jnp.arange(4 * padded, dtype=jnp.int32) % padded)[None, :]

    w_q, w_k, w_v, context = spread(blocks_a, r, (slot,), 1)
    x = tokens.astype(f32)
    n1, z1 = unit_rows(x)
    a1 = (n1 * gain_self).astype(bf16)
    n1_context = unit_rows(context.astype(f32))[0]
    a1_context = (n1_context * gain_self).astype(bf16)
    a1_all = settle(jnp.concatenate([a1_context, a1]))
    q = nt(a1, w_q, bf16)
    k = nt(a1_all, w_k, bf16)
    v = nt(a1_all, w_v, bf16)
    o, lse = self_attention(q, k, v, at_self, lim, 2)
    w_o, w_cq, w_ck, w_cv, w_co, e = spread(blocks_b, r, (piece, other), 2)
    h1 = x + nn(o, w_o)

    n2, z2 = unit_rows(h1)
    a2 = (n2 * gain_cross).astype(bf16)
    cq = nt(a2, w_cq, bf16)
    ck = nt(e, w_ck, bf16)
    cv = nt(e, w_cv, bf16)
    oc, lse_c = cross_attention(cq, ck, cv, at_cross, frames, 2)
    h2 = h1 + nn(oc, w_co)

    (w_up,) = spread(blocks_c, rf, (), 3)
    (w_down,) = spread(blocks_f, rf, (), 4)
    n3, z3 = unit_rows(h2)
    a3 = (n3 * gain_hidden).astype(bf16)
    u = nt(a3, w_up)
    g = jax.nn.gelu(u, approximate=False).astype(bf16)
    h3 = h2 + nn(g, w_down)
    n4, z4 = unit_rows(h3)
    layer_out = (n4 * gain_final).astype(bf16)

    c3 = cotangent.astype(f32)
    gain_4 = jnp.sum(c3 * n4, axis=0)
    dh3 = norm_back(n4, z4, gain_final, c3)
    db3 = dh3.astype(bf16)
    g_down = tn(g, db3, bf16)
    (s_down,) = reduce_weights([g_down])
    _, gelu_pull = jax.vjp(lambda t: jax.nn.gelu(t, approximate=False), u)
    through = nt(db3, w_down)
    du = gelu_pull(through)[0].astype(bf16)
    g_up = tn(du, a3, bf16)
    (s_up,) = reduce_weights([g_up])
    da3 = nn(du, w_up)
    gain_3 = jnp.sum(da3 * n3, axis=0)
    dh2 = dh3 + norm_back(n3, z3, gain_hidden, da3)
    db2 = dh2.astype(bf16)

    g_co = tn(oc, db2, bf16)
    doc = nt(db2, w_co, bf16)
    dcq, dck, dcv = cross_attention_back(cq, doc, oc, lse_c, ck, cv, at_cross, frames, 3)
    g_cq = tn(dcq, a2, bf16)
    g_ck = tn(dck, e, bf16)
    g_cv = tn(dcv, e, bf16)
    de = (nn(dck, w_ck) + nn(dcv, w_cv)).astype(bf16)
    two = 2 * padded
    de = add(de[:two], flip(de[two:], "row", 1))
    grad_encoded = de[:padded].astype(f32) + flip(de[padded:], "row", 2).astype(f32)
    grad_encoded = grad_encoded[:frames]
    da2 = nn(dcq, w_cq)
    gain_2 = jnp.sum(da2 * n2, axis=0)
    dh1 = dh2 + norm_back(n2, z2, gain_cross, da2)
    db1 = dh1.astype(bf16)

    g_o = tn(o, db1, bf16)
    s_o, s_cq, s_ck, s_cv, s_co = reduce_weights([g_o, g_cq, g_ck, g_cv, g_co])
    do = nt(db1, w_o, bf16)
    dq, dk, dv = self_attention_back(q, do, o, lse, k, v, at_self, lim, 3)
    da_all = nn(dk, w_k) + nn(dv, w_v)
    ctx = PROMPT
    part = da_all[:ctx]
    own = nn(dq, w_q) + da_all[ctx:]
    gain_1 = jnp.sum(own * n1, axis=0) + jnp.sum(part * n1_context, axis=0)
    mine = part[: ctx // 2]
    mine = mine + flip(part[ctx // 2 :].astype(bf16), "row", 1).astype(f32)
    back = lax.ppermute(mine.astype(bf16), "row", [(2, 0), (3, 1)]).astype(f32)
    gains = sum_all(jnp.stack([gain_1, gain_2, gain_3, gain_4]))
    g_q = tn(dq, a1, bf16)
    g_k = tn(dk, a1_all, bf16)
    g_v = tn(dv, a1_all, bf16)
    s_q, s_k, s_v = reduce_weights([g_q, g_k, g_v])
    da1 = own + jnp.where(row < 2, mine + back, 0.0)
    grad_tokens = dh1 + norm_back(n1, z1, gain_self, da1)

    return (
        layer_out,
        grad_tokens,
        grad_encoded,
        gains[0],
        s_q.T,
        s_k.T,
        s_v.T,
        s_o,
        gains[1],
        s_cq.T,
        s_ck.T,
        s_cv.T,
        s_co,
        gains[2],
        s_up.T,
        s_down,
        gains[3],
    )


def solution(mesh):
    rows = P(("dp", "col", "row"), None)
    down, across_ = P("col", "row"), P("row", "col")
    return jax.shard_map(
        layer,
        mesh=mesh,
        in_specs=(
            rows, rows, P(("dp", "col"), None), rows,
            P(), down, down, down, across_,
            P(), down, down, down, across_,
            P(), down, across_, P(),
        ),
        out_specs=(
            rows, rows, rows,
            P(), down, down, down, across_,
            P(), down, down, down, across_,
            P(), down, across_, P(),
        ),
        check_vma=False,
    )
```

```python
import functools

import jax
import jax.numpy as jnp
from jax import lax
from jax.experimental import pallas as pl
from jax.experimental.pallas import tpu as pltpu
from jax.sharding import PartitionSpec as P


HEAD_DIM = 64
PROMPT = 1024
CONT = 256
NCONT = 4
PAIR = 2 * HEAD_DIM
LOG2E = 1.4426950408889634

eps = 1e-05
big_neg = -1e30
bf16 = jnp.bfloat16
f32 = jnp.float32


def dot(left, right, contract, dtype=f32):
    out = lax.dot_general(left, right, (contract, ((), ())), preferred_element_type=f32)
    return out.astype(dtype)


def nn(left, right, dtype=f32):
    return dot(left, right, ((1,), (0,)), dtype)


def nt(left, right, dtype=f32):
    return dot(left, right, ((1,), (1,)), dtype)


def tn(left, right, dtype=f32):
    return dot(left, right, ((0,), (0,)), dtype)


def unit_rows(rows_in):
    average = jnp.mean(rows_in, axis=-1, keepdims=True)
    centred = rows_in - average
    variance = jnp.mean(centred * centred, axis=-1, keepdims=True)
    scale = lax.rsqrt(variance + eps)
    return centred * scale, scale


def norm_back(unit, scale, gain, upstream):
    cw = upstream * gain
    first = jnp.mean(cw, axis=-1, keepdims=True)
    second = jnp.mean(cw * unit, axis=-1, keepdims=True)
    return scale * (cw - first - unit * second)


def head_masks(rows):
    lane = lax.broadcasted_iota(jnp.int32, (rows, PAIR), 1)
    return (lane < HEAD_DIM, lane >= HEAD_DIM)


def masked_scores(q, keys, limits):
    out = []
    for k, limit in zip(keys, limits):
        s = nt(q, k) * LOG2E
        if limit is not None:
            where, bound = limit
            s = jnp.where(where < bound, s, big_neg)
        out.append(s)
    return out


def fwd_body(q_ref, kv_refs, limits, o_ref, lse_ref):
    rows = q_ref.shape[0]
    masks = head_masks(rows)
    q = q_ref[...] * jnp.asarray(HEAD_DIM**-0.5, bf16)
    keys = [k[...] for k, _ in kv_refs]
    values = [v[...] for _, v in kv_refs]
    blended, logs = [], []
    for mask in masks:
        scores = masked_scores(jnp.where(mask, q, 0), keys, limits)
        top = functools.reduce(
            jnp.maximum, [jnp.max(s, axis=-1, keepdims=True) for s in scores]
        )
        raised = [jnp.exp2(s - top) for s in scores]
        total = functools.reduce(
            jnp.add, [jnp.sum(p, axis=-1, keepdims=True) for p in raised]
        )
        mixed = functools.reduce(
            jnp.add, [nn(p.astype(bf16), v) for p, v in zip(raised, values)]
        )
        blended.append(mixed / total)
        logs.append(top + jnp.log2(total))
    o_ref[...] = jnp.where(masks[0], blended[0], blended[1]).astype(bf16)
    lse_ref[...] = jnp.where(masks[0], logs[0], logs[1])


def bwd_body(q_ref, do_ref, o_ref, lse_ref, kv_refs, limits, dq_ref):
    rows = q_ref.shape[0]
    masks = head_masks(rows)
    q = q_ref[...] * jnp.asarray(HEAD_DIM**-0.5, bf16)
    grad = do_ref[...]
    product = grad.astype(f32) * o_ref[...].astype(f32)
    lse = lse_ref[...]
    keys = [k[...] for k, _ in kv_refs]
    values = [v[...] for _, v in kv_refs]
    sums_k = [None] * len(keys)
    sums_v = [None] * len(keys)
    grads_q = []
    for h, mask in enumerate(masks):
        qh = jnp.where(mask, q, 0)
        gh = jnp.where(mask, grad, 0)
        delta = jnp.sum(jnp.where(mask, product, 0), axis=-1, keepdims=True)
        level = lse[:, h * HEAD_DIM : h * HEAD_DIM + 1]
        scores = masked_scores(qh, keys, limits)
        grad_q = None
        for i, s in enumerate(scores):
            p = jnp.exp2(s - level)
            through = nt(gh, values[i])
            slope = (p * (through - delta)).astype(bf16)
            part = nn(slope, keys[i])
            grad_q = part if grad_q is None else grad_q + part
            dk, dv = tn(qh, slope), tn(gh, p.astype(bf16))
            sums_k[i] = dk if sums_k[i] is None else sums_k[i] + dk
            sums_v[i] = dv if sums_v[i] is None else sums_v[i] + dv
        grads_q.append(grad_q)
    mixed = jnp.where(masks[0], grads_q[0], grads_q[1]) * HEAD_DIM**-0.5
    dq_ref[...] = mixed.astype(bf16)
    return sums_k, sums_v


def self_fwd_kernel(q_ref, kc_ref, vc_ref, ko_ref, vo_ref, at_ref, lim_ref, o_ref, lse_ref):
    lim = lim_ref[...]
    own = lax.broadcasted_iota(jnp.int32, (1, ko_ref.shape[0]), 1)
    limits = [(at_ref[...], lim[:, 0:1]), (own, lim[:, 1:2])]
    fwd_body(q_ref, [(kc_ref, vc_ref), (ko_ref, vo_ref)], limits, o_ref, lse_ref)


def cross_fwd_kernel(q_ref, k_ref, v_ref, at_ref, o_ref, lse_ref, *, frames):
    limits = [(at_ref[...], frames)]
    fwd_body(q_ref, [(k_ref, v_ref)], limits, o_ref, lse_ref)


def self_bwd_kernel(
    q_ref, do_ref, o_ref, lse_ref, kc_ref, vc_ref, ko_ref, vo_ref, at_ref, lim_ref,
    dq_ref, dk_ref, dv_ref, dk_acc, dv_acc,
):
    step = pl.program_id(1)
    last = pl.num_programs(1) - 1
    ctx = kc_ref.shape[0]
    block = ko_ref.shape[0]
    lim = lim_ref[...]
    own = lax.broadcasted_iota(jnp.int32, (1, block), 1)
    limits = [(at_ref[...], lim[:, 0:1]), (own, lim[:, 1:2])]
    sums_k, sums_v = bwd_body(
        q_ref, do_ref, o_ref, lse_ref, [(kc_ref, vc_ref), (ko_ref, vo_ref)], limits, dq_ref
    )
    at = pl.multiple_of(ctx + step * block, block)
    dk_ref[pl.ds(at, block), :] = sums_k[1].T.astype(bf16)
    dv_ref[pl.ds(at, block), :] = sums_v[1].T.astype(bf16)

    @pl.when(step == 0)
    def _():
        dk_acc[...] = sums_k[0]
        dv_acc[...] = sums_v[0]

    @pl.when(step > 0)
    def _():
        dk_acc[...] += sums_k[0]
        dv_acc[...] += sums_v[0]

    @pl.when(step == last)
    def _():
        dk_ref[0:ctx, :] = dk_acc[...].T.astype(bf16)
        dv_ref[0:ctx, :] = dv_acc[...].T.astype(bf16)


def cross_bwd_kernel(
    q_ref, do_ref, o_ref, lse_ref, k_ref, v_ref, at_ref,
    dq_ref, dk_ref, dv_ref, dk_acc, dv_acc, *, frames,
):
    step = pl.program_id(1)
    last = pl.num_programs(1) - 1
    sums_k, sums_v = bwd_body(
        q_ref, do_ref, o_ref, lse_ref, [(k_ref, v_ref)], [(at_ref[...], frames)], dq_ref
    )

    @pl.when(step == 0)
    def _():
        dk_acc[...] = sums_k[0]
        dv_acc[...] = sums_v[0]

    @pl.when(step > 0)
    def _():
        dk_acc[...] += sums_k[0]
        dv_acc[...] += sums_v[0]

    @pl.when(step == last)
    def _():
        dk_ref[...] = dk_acc[...].T.astype(bf16)
        dv_ref[...] = dv_acc[...].T.astype(bf16)


def params():
    return pltpu.CompilerParams(
        dimension_semantics=("arbitrary", "arbitrary"), vmem_limit_bytes=56 * 2**20
    )


def cost(rows, keys, width, matmuls):
    return pl.CostEstimate(
        flops=2 * matmuls * rows * keys * width * 4,
        transcendentals=rows * keys * width // HEAD_DIM,
        bytes_accessed=2 * width * (4 * rows + 4 * keys),
    )


def in_parts(kernel, parts, width, ins, specs, out_specs, shapes, scratch, grid_rows, estimate):
    pairs = width // PAIR
    step = pairs // parts
    outs = None
    for i in range(parts):
        first = i * step

        def moved(spec, first=first):
            if spec is None:
                return pl.BlockSpec(memory_space=pl.ANY)
            block, index = spec
            return pl.BlockSpec(block, lambda p, b: index(p + first, b))

        given = list(ins) + (list(outs) if outs else [])
        extra = len(outs) if outs else 0

        def body(*refs, extra=extra):
            kernel(*refs[: len(ins)], *refs[len(ins) + extra :])

        outs = pl.pallas_call(
            body,
            grid=(step, grid_rows),
            in_specs=[moved(spec) for spec in specs] + [moved(None)] * extra,
            out_specs=[moved(spec) for spec in out_specs],
            out_shape=shapes,
            scratch_shapes=scratch,
            input_output_aliases={len(ins) + j: j for j in range(extra)},
            compiler_params=params(),
            cost_estimate=estimate(width // parts),
        )(*given)
    return outs


def q_spec(block):
    return ((block, PAIR), lambda p, b: (b, p))


def sds(rows, width, kind):
    return jax.ShapeDtypeStruct((rows, width), kind)


def self_specs(ctx):
    first = ctx // CONT
    context = ((ctx, PAIR), lambda p, b: (0, p))
    own = ((CONT, PAIR), lambda p, b: (first + b, p))
    return [
        context, context, own, own,
        ((1, ctx), lambda p, b: (0, 0)),
        ((CONT, 2), lambda p, b: (b, 0)),
    ]


def self_attention(q, k, v, at, lim, parts):
    rows, width = q.shape
    ctx = k.shape[0] - rows
    return in_parts(
        self_fwd_kernel, parts, width,
        (q, k, v, k, v, at, lim), [q_spec(CONT)] + self_specs(ctx),
        [q_spec(CONT)] * 2, [sds(rows, width, bf16), sds(rows, width, f32)], [],
        rows // CONT, lambda w: cost(rows, ctx + CONT, w, 2),
    )


def self_attention_back(q, do, o, lse, k, v, at, lim, parts):
    rows, width = q.shape
    ctx = k.shape[0] - rows
    whole = ((ctx + rows, PAIR), lambda p, b: (0, p))
    return in_parts(
        self_bwd_kernel, parts, width,
        (q, do, o, lse, k, v, k, v, at, lim), [q_spec(CONT)] * 4 + self_specs(ctx),
        [q_spec(CONT), whole, whole],
        [sds(rows, width, bf16), sds(ctx + rows, width, bf16), sds(ctx + rows, width, bf16)],
        [pltpu.VMEM((PAIR, ctx), f32), pltpu.VMEM((PAIR, ctx), f32)],
        rows // CONT, lambda w: cost(rows, ctx + CONT, w, 5),
    )


def cross_attention(q, k, v, at, frames, parts):
    rows, width = q.shape
    keys = k.shape[0]
    whole = ((keys, PAIR), lambda p, b: (0, p))
    return in_parts(
        functools.partial(cross_fwd_kernel, frames=frames), parts, width,
        (q, k, v, at), [q_spec(CONT), whole, whole, ((1, keys), lambda p, b: (0, 0))],
        [q_spec(CONT)] * 2, [sds(rows, width, bf16), sds(rows, width, f32)], [],
        rows // CONT, lambda w: cost(rows, keys, w, 2),
    )


def cross_attention_back(q, do, o, lse, k, v, at, frames, parts):
    rows, width = q.shape
    keys = k.shape[0]
    whole = ((keys, PAIR), lambda p, b: (0, p))
    return in_parts(
        functools.partial(cross_bwd_kernel, frames=frames), parts, width,
        (q, do, o, lse, k, v, at),
        [q_spec(CONT)] * 4 + [whole, whole, ((1, keys), lambda p, b: (0, 0))],
        [q_spec(CONT), whole, whole],
        [sds(rows, width, bf16), sds(keys, width, bf16), sds(keys, width, bf16)],
        [pltpu.VMEM((PAIR, keys), f32), pltpu.VMEM((PAIR, keys), f32)],
        rows // CONT, lambda w: cost(rows, keys, w, 5),
    )


def up_kernel(a_ref, w_ref, g_ref, slope_ref):
    u = nt(a_ref[...], w_ref[...])
    share = 0.5 * (1.0 + lax.erf(u * 0.7071067811865476))
    density = jnp.exp2(u * u * (-0.5 * LOG2E)) * 0.3989422804014327
    g_ref[...] = (u * share).astype(bf16)
    slope_ref[...] = (share + u * density).astype(bf16)


def feed_up(a, w):
    rows, width = a.shape
    hidden = w.shape[0]
    block = 512
    out = pl.BlockSpec((rows, block), lambda i: (0, i))
    return pl.pallas_call(
        up_kernel,
        grid=(hidden // block,),
        in_specs=[
            pl.BlockSpec((rows, width), lambda i: (0, 0)),
            pl.BlockSpec((block, width), lambda i: (i, 0)),
        ],
        out_specs=[out, out],
        out_shape=[sds(rows, hidden, bf16)] * 2,
        compiler_params=pltpu.CompilerParams(vmem_limit_bytes=40 * 2**20),
        cost_estimate=pl.CostEstimate(
            flops=2 * rows * width * hidden,
            transcendentals=2 * rows * hidden,
            bytes_accessed=2 * (hidden * width + rows * width + 2 * rows * hidden),
        ),
        name="feed_up",
    )(a, w)


def flip(value, axis, bit):
    size = lax.axis_size(axis)
    return lax.ppermute(value, axis, [(i, i ^ bit) for i in range(size)])


def bits(axis):
    size = lax.axis_size(axis)
    return [1 << b for b in range(size.bit_length() - 1)]


def settle(value):
    return lax.optimization_barrier(value)


def pack_kernel(turned, *refs):
    out, at = refs[-1], 0
    for ref, turn in zip(refs[:-1], turned):
        value = ref[...]
        if turn:
            value = value.astype(f32).T.astype(bf16)
        out[at : at + value.shape[0], :] = value
        at += value.shape[0]


def pack(weights, turned):
    rows = sum(w.shape[1] if t else w.shape[0] for w, t in zip(weights, turned))
    width = weights[0].shape[0] if turned[0] else weights[0].shape[1]
    if width % 128:
        return jnp.concatenate([w.T if t else w for w, t in zip(weights, turned)])
    return pl.pallas_call(
        functools.partial(pack_kernel, turned),
        out_shape=sds(rows, width, bf16),
        grid=(1,),
        in_specs=[pl.BlockSpec(w.shape, lambda i: (0, 0)) for w in weights],
        out_specs=pl.BlockSpec((rows, width), lambda i: (0, 0)),
        compiler_params=pltpu.CompilerParams(vmem_limit_bytes=16 * 2**20),
        cost_estimate=pl.CostEstimate(flops=0, transcendentals=0, bytes_accessed=4 * rows * width),
        name="pack",
    )(*weights)


def col_order(parts):
    count = len(parts)
    place = lax.axis_index("col")
    if count == 1:
        return parts
    if count == 2:
        even = place == 0
        return [jnp.where(even, parts[0], parts[1]), jnp.where(even, parts[1], parts[0])]
    stacked = jnp.stack(parts)
    return [stacked[jnp.bitwise_xor(place, a)] for a in range(count)]


def near_blocks(shard):
    near = [[shard], [flip(shard, "row", 2)]]
    for bit in bits("col"):
        near = [list(p) + [flip(block, "col", bit) for block in p] for p in near]
    return near


def spread_kernel(r, count, plain, *refs):
    sources = refs[: 4 + len(plain)]
    outs = refs[4 + len(plain) : 4 + len(plain) + count + (1 if plain else 0)]
    rest = refs[4 + len(plain) + count + (1 if plain else 0) :]
    buffers, (in_sem, out_sem, send_sem, recv_sem) = rest[:-4], rest[-4:]
    width = sources[0].shape[1]
    me = lax.axis_index("row")
    partner = {"row": me + 1 - 2 * lax.rem(me, 2)}
    place = lax.axis_index("col")

    barrier = pltpu.get_barrier_semaphore()
    pl.semaphore_signal(barrier, inc=1, device_id=partner, device_id_type=pl.DeviceIdType.MESH)
    loads = []
    for i, source in enumerate(sources):
        buffer = buffers[0].at[i] if i < 4 else buffers[1].at[i - 4]
        load = pltpu.make_async_copy(source, buffer, in_sem.at[i])
        load.start()
        loads.append(load)
    pl.semaphore_wait(barrier, 1)
    waits, n = [], 0

    def place_both(piece, here, there):
        nonlocal n
        local_copy = pltpu.make_async_copy(piece, here, out_sem.at[n])
        remote_copy = pltpu.make_async_remote_copy(
            src_ref=piece, dst_ref=there, send_sem=send_sem.at[n], recv_sem=recv_sem.at[n],
            device_id=partner, device_id_type=pl.DeviceIdType.MESH,
        )
        local_copy.start()
        remote_copy.start()
        waits.append((local_copy, remote_copy))
        n += 1

    for i in range(4):
        p, j = i // 2, i % 2
        loads[i].wait()
        side = place if j == 0 else 1 - place
        lanes = pl.ds(pl.multiple_of(side * width, 128), width)
        for w in range(count):
            piece = buffers[0].at[i, pl.ds(w * r, r), :]
            place_both(
                piece,
                outs[w].at[pl.ds(p * r, r), lanes],
                outs[w].at[pl.ds((p + 2) * r, r), lanes],
            )
    for i, rows in enumerate(plain):
        loads[4 + i].wait()
        place_both(
            buffers[1].at[i],
            outs[count].at[pl.ds(i * rows, rows), :],
            outs[count].at[pl.ds((len(plain) + i) * rows, rows), :],
        )
    for local_copy, remote_copy in waits:
        local_copy.wait()
        remote_copy.wait()


def spread(blocks, r, plain, number):
    rows, width = blocks[0][0].shape
    count = rows // r
    if lax.axis_size("col") != 2 or width % 128:
        every = blocks + [[flip(b, "row", 1) for b in p] for p in blocks]
        outs = [
            jnp.concatenate(
                [
                    jnp.concatenate(col_order([b[w * r : (w + 1) * r] for b in p]), axis=1)
                    for p in every
                ]
            )
            for w in range(count)
        ]
        if plain:
            outs.append(jnp.concatenate(list(plain) + [flip(x, "row", 1) for x in plain]))
        return outs
    flat = [b for p in blocks for b in p]
    moves = 4 * count + len(plain)
    shapes = [sds(4 * r, 2 * width, bf16)] * count
    scratch = [pltpu.VMEM((4, rows, width), bf16)]
    if plain:
        n, wide = plain[0].shape
        shapes = shapes + [sds(2 * len(plain) * n, wide, bf16)]
        scratch.append(pltpu.VMEM((len(plain), n, wide), bf16))
    any_place = pl.BlockSpec(memory_space=pl.ANY)
    return pl.pallas_call(
        functools.partial(spread_kernel, r, count, tuple(x.shape[0] for x in plain)),
        out_shape=shapes,
        in_specs=[any_place] * (4 + len(plain)),
        out_specs=[any_place] * len(shapes),
        scratch_shapes=scratch
        + [
            pltpu.SemaphoreType.DMA((4 + len(plain),)),
            pltpu.SemaphoreType.DMA((moves,)),
            pltpu.SemaphoreType.DMA((moves,)),
            pltpu.SemaphoreType.DMA((moves,)),
        ],
        compiler_params=pltpu.CompilerParams(
            collective_id=number, has_side_effects=True, vmem_limit_bytes=24 * 2**20
        ),
        cost_estimate=pl.CostEstimate(flops=0, transcendentals=0, bytes_accessed=24 * rows * width),
    )(*flat, *plain)


def col_halves(value):
    count = lax.axis_size("col")
    width = value.shape[1] // count
    return [value[:, i * width : (i + 1) * width] for i in range(count)]


def add(a, b):
    return (a.astype(f32) + b.astype(f32)).astype(bf16)


def reduce_weights(grads):
    kept = []
    for g in grads:
        half = g.shape[0] // 2
        kept.append(add(g[:half], flip(g[half:], "row", 1)))
    sizes = [k.shape[0] // 2 for k in kept]
    joined = jnp.concatenate(
        [k[:s] for k, s in zip(kept, sizes)] + [k[s:] for k, s in zip(kept, sizes)]
    )
    parts = col_order(col_halves(joined))
    for bit in reversed(bits("col")):
        keep, send = parts[:bit], parts[bit:]
        parts = [add(a, flip(b, "col", bit)) for a, b in zip(keep, send)]
    total = parts[0]
    half = total.shape[0] // 2
    total = settle(add(total[:half], flip(total[half:], "row", 2)))
    for bit in bits("dp")[:-1]:
        total = settle(add(total, flip(total, "dp", bit)))
    last = bits("dp")[-1]
    total = total.astype(f32) + flip(total, "dp", last).astype(f32)
    out, at = [], 0
    for s in sizes:
        out.append(total[at : at + s])
        at += s
    return out


def sum_all(value):
    for axis, bit in [("row", 1), ("col", None), ("row", 2), ("dp", None)]:
        for b in bits(axis) if bit is None else [bit]:
            value = value + flip(value, axis, b)
    return value


def finish_kernel(
    gq_ref, gk_ref, gv_ref, part_ref, gains_ref,
    q_out, k_out, v_out, back_out, gains_out,
    c_recv, c_part, y_send, y_recv, y_keep, x_send, x_recv, z_send, z_recv,
    p_send, p_recv, g_send, g_recv, send_sem, recv_sem,
):
    grads = (gq_ref, gk_ref, gv_ref)
    outs = (q_out, k_out, v_out)
    me, place, depth = lax.axis_index("row"), lax.axis_index("col"), lax.axis_index("dp")
    core = {"row": me + 1 - 2 * lax.rem(me, 2)}
    across_x = {"row": lax.rem(me + 2, 4)}
    across_y = {"col": 1 - place}
    near_z = {"dp": depth + 1 - 2 * lax.rem(depth, 2)}
    far_z = {"dp": lax.rem(depth + 2, 4)}
    partners = (core, across_y, across_x, near_z, far_z)
    half = gq_ref.shape[0] // 2
    r = half // 2
    lanes = gq_ref.shape[1] // 2
    rows = back_out.shape[0]
    mine = pl.ds(pl.multiple_of(place * lanes, 128), lanes)
    theirs = pl.ds(pl.multiple_of((1 - place) * lanes, 128), lanes)

    barrier = pltpu.get_barrier_semaphore()
    for partner in partners:
        pl.semaphore_signal(barrier, inc=1, device_id=partner, device_id_type=pl.DeviceIdType.MESH)
    pl.semaphore_wait(barrier, len(partners))
    started = []

    def send(source, target, partner):
        n = len(started)
        copy = pltpu.make_async_remote_copy(
            src_ref=source, dst_ref=target, send_sem=send_sem.at[n], recv_sem=recv_sem.at[n],
            device_id=partner, device_id_type=pl.DeviceIdType.MESH,
        )
        copy.start()
        started.append(copy)
        return copy

    gain = send(gains_ref, g_recv.at[0], core)
    part = send(part_ref.at[pl.ds(rows, rows)], c_part, core)
    hops = [
        send(g.at[pl.ds(half, half)], c_recv.at[w], core) for w, g in enumerate(grads)
    ]

    def pass_gain(copy, n, value, partner):
        copy.wait_recv()
        value = value + g_recv[n]
        g_send[n] = value
        return value, send(g_send.at[n], g_recv.at[n + 1], partner)

    total, gain = pass_gain(gain, 0, gains_ref[...], across_y)
    part.wait_recv()
    p_send[...] = (part_ref[0:rows, :].astype(f32) + c_part[...].astype(f32)).astype(bf16)
    for w, g in enumerate(grads):
        hops[w].wait_recv()
        y_send[w] = (
            g[0:half, theirs].astype(f32) + c_recv[w, :, theirs].astype(f32)
        ).astype(bf16)
        hops[w] = send(y_send.at[w], y_recv.at[w], across_y)
        if w == 0:
            part = send(p_send, p_recv, across_x)
        y_keep[w] = g[0:half, mine].astype(f32) + c_recv[w, :, mine].astype(f32)
    total, gain = pass_gain(gain, 1, total, across_x)
    for w in range(3):
        hops[w].wait_recv()
        x_send[w] = (y_keep[w, r:half, :] + y_recv[w, r:half, :].astype(f32)).astype(bf16)
        hops[w] = send(x_send.at[w], x_recv.at[w], across_x)
        y_keep[w, 0:r, :] = y_keep[w, 0:r, :] + y_recv[w, 0:r, :].astype(f32)
    part.wait_recv()
    keep = jnp.where(me < 2, 1.0, 0.0)
    back_out[...] = keep * (p_send[...].astype(f32) + p_recv[...].astype(f32))
    total, gain = pass_gain(gain, 2, total, near_z)
    for w in range(3):
        hops[w].wait_recv()
        z_send[0, w] = (y_keep[w, 0:r, :] + x_recv[w].astype(f32)).astype(bf16)
        hops[w] = send(z_send.at[0, w], z_recv.at[0, w], near_z)
    total, gain = pass_gain(gain, 3, total, far_z)
    for w in range(3):
        hops[w].wait_recv()
        z_send[1, w] = (z_send[0, w].astype(f32) + z_recv[0, w].astype(f32)).astype(bf16)
        hops[w] = send(z_send.at[1, w], z_recv.at[1, w], far_z)
    gain.wait_recv()
    gains_out[...] = total + g_recv[4]
    for w in range(3):
        hops[w].wait_recv()
        outs[w][...] = z_send[1, w].astype(f32) + z_recv[1, w].astype(f32)
    for copy in started:
        copy.wait_send()


def finish(grads, part, gains):
    full, width = grads[0].shape
    half, r, lanes = full // 2, full // 4, width // 2
    rows = part.shape[0] // 2
    count = 5 * 4 + 2
    return pl.pallas_call(
        finish_kernel,
        out_shape=[sds(r, lanes, f32)] * 3 + [sds(rows, width, f32), sds(8, width, f32)],
        in_specs=[pl.BlockSpec(memory_space=pltpu.VMEM)] * 5,
        out_specs=[pl.BlockSpec(memory_space=pltpu.VMEM)] * 5,
        scratch_shapes=[
            pltpu.VMEM((3, half, width), bf16),
            pltpu.VMEM((rows, width), bf16),
            pltpu.VMEM((3, half, lanes), bf16),
            pltpu.VMEM((3, half, lanes), bf16),
            pltpu.VMEM((3, half, lanes), f32),
            pltpu.VMEM((3, r, lanes), bf16),
            pltpu.VMEM((3, r, lanes), bf16),
            pltpu.VMEM((2, 3, r, lanes), bf16),
            pltpu.VMEM((2, 3, r, lanes), bf16),
            pltpu.VMEM((rows, width), bf16),
            pltpu.VMEM((rows, width), bf16),
            pltpu.VMEM((4, 8, width), f32),
            pltpu.VMEM((5, 8, width), f32),
            pltpu.SemaphoreType.DMA((count,)),
            pltpu.SemaphoreType.DMA((count,)),
        ],
        compiler_params=pltpu.CompilerParams(
            collective_id=5, has_side_effects=True, vmem_limit_bytes=40 * 2**20
        ),
        cost_estimate=pl.CostEstimate(
            flops=0, transcendentals=0, bytes_accessed=100 * 2**20
        ),
        name="finish",
    )(*grads, part, gains)


def layer(
    tokens,
    encoded,
    branch,
    cotangent,
    gain_self,
    self_query,
    self_key,
    self_value,
    self_out,
    gain_cross,
    cross_query,
    cross_key,
    cross_value,
    cross_out,
    gain_hidden,
    hidden_up,
    hidden_down,
    gain_final,
):
    row = lax.axis_index("row")
    rows, _ = tokens.shape
    frames = encoded.shape[0]
    padded = -(-frames // 128) * 128
    r = self_query.shape[1]
    rf = hidden_up.shape[1]

    blocks_a = near_blocks(pack((self_query, self_key, self_value), (True, True, True)))
    moved = lax.ppermute(tokens, "row", [(0, 2), (1, 3)])
    slot = jnp.where(row < 2, tokens, moved)
    blocks_b = near_blocks(
        pack(
            (self_out, cross_query, cross_key, cross_value, cross_out),
            (False, True, True, True, False),
        ),
    )
    piece = jnp.pad(encoded, ((0, padded - frames), (0, 0)))
    other = flip(piece, "row", 2)
    blocks_c = near_blocks(pack((hidden_up,), (True,)))
    blocks_f = near_blocks(hidden_down)

    position = row * rows + jnp.arange(rows, dtype=jnp.int32)
    chosen = (position - PROMPT) // CONT
    chosen = (chosen[:, None] == jnp.arange(NCONT, dtype=jnp.int32)[None, :]).astype(jnp.int32)
    cut = jnp.sum(chosen * branch[0][None, :], axis=1)
    is_prompt = position < PROMPT
    lim = jnp.stack(
        [
            jnp.where(is_prompt, position + 1, cut),
            jnp.where(is_prompt, 0, position % CONT + 1),
        ],
        axis=1,
    )
    offsets = jnp.arange(rows, dtype=jnp.int32)
    side = jnp.bitwise_and(row, 1)
    at_self = jnp.concatenate([side * rows + offsets, (1 - side) * rows + offsets])[None, :]
    at_cross = (jnp.arange(4 * padded, dtype=jnp.int32) % padded)[None, :]

    w_q, w_k, w_v, context = spread(blocks_a, r, (slot,), 1)
    x = tokens.astype(f32)
    n1, z1 = unit_rows(x)
    a1 = (n1 * gain_self).astype(bf16)
    n1_context = unit_rows(context.astype(f32))[0]
    a1_context = (n1_context * gain_self).astype(bf16)
    a1_all = settle(jnp.concatenate([a1_context, a1]))
    q = nt(a1, w_q, bf16)
    k = nt(a1_all, w_k, bf16)
    v = nt(a1_all, w_v, bf16)
    o, lse = self_attention(q, k, v, at_self, lim, 2)
    w_o, w_cq, w_ck, w_cv, w_co, e = spread(blocks_b, r, (piece, other), 2)
    h1 = x + nn(o, w_o)

    n2, z2 = unit_rows(h1)
    a2 = (n2 * gain_cross).astype(bf16)
    cq = nt(a2, w_cq, bf16)
    ck = nt(e, w_ck, bf16)
    cv = nt(e, w_cv, bf16)
    oc, lse_c = cross_attention(cq, ck, cv, at_cross, frames, 2)
    h2 = h1 + nn(oc, w_co)

    (w_up,) = spread(blocks_c, rf, (), 3)
    (w_down,) = spread(blocks_f, rf, (), 4)
    n3, z3 = unit_rows(h2)
    a3 = (n3 * gain_hidden).astype(bf16)
    g, slope = feed_up(a3, w_up)
    h3 = h2 + nn(g, w_down)
    n4, z4 = unit_rows(h3)
    layer_out = (n4 * gain_final).astype(bf16)

    c3 = cotangent.astype(f32)
    gain_4 = jnp.sum(c3 * n4, axis=0)
    dh3 = norm_back(n4, z4, gain_final, c3)
    db3 = dh3.astype(bf16)
    g_down = tn(g, db3, bf16)
    (s_down,) = reduce_weights([g_down])
    through = nt(db3, w_down)
    du = (through * slope.astype(f32)).astype(bf16)
    g_up = tn(du, a3, bf16)
    da3 = nn(du, w_up)
    gain_3 = jnp.sum(da3 * n3, axis=0)
    dh2 = dh3 + norm_back(n3, z3, gain_hidden, da3)
    db2 = dh2.astype(bf16)

    g_co = tn(oc, db2, bf16)
    s_up, s_co = reduce_weights([g_up, g_co])
    doc = nt(db2, w_co, bf16)
    dcq, dck, dcv = cross_attention_back(cq, doc, oc, lse_c, ck, cv, at_cross, frames, 3)
    g_cq = tn(dcq, a2, bf16)
    g_ck = tn(dck, e, bf16)
    g_cv = tn(dcv, e, bf16)
    de = (nn(dck, w_ck) + nn(dcv, w_cv)).astype(bf16)
    two = 2 * padded
    de = add(de[:two], flip(de[two:], "row", 1))
    grad_encoded = de[:padded].astype(f32) + flip(de[padded:], "row", 2).astype(f32)
    grad_encoded = grad_encoded[:frames]
    da2 = nn(dcq, w_cq)
    gain_2 = jnp.sum(da2 * n2, axis=0)
    dh1 = dh2 + norm_back(n2, z2, gain_cross, da2)
    db1 = dh1.astype(bf16)

    g_o = tn(o, db1, bf16)
    s_o, s_cq, s_ck, s_cv = reduce_weights([g_o, g_cq, g_ck, g_cv])
    do = nt(db1, w_o, bf16)
    dq, dk, dv = self_attention_back(q, do, o, lse, k, v, at_self, lim, 3)
    da_all = nn(dk, w_k) + nn(dv, w_v)
    ctx = PROMPT
    part = da_all[:ctx]
    own = nn(dq, w_q) + da_all[ctx:]
    gain_1 = jnp.sum(own * n1, axis=0) + jnp.sum(part * n1_context, axis=0)
    part = part.astype(bf16)
    gains = jnp.stack([gain_1, gain_2, gain_3, gain_4])
    g_q = tn(dq, a1, bf16)
    g_k = tn(dk, a1_all, bf16)
    g_v = tn(dv, a1_all, bf16)
    sizes = (lax.axis_size("row"), lax.axis_size("col"), lax.axis_size("dp"))
    if sizes == (4, 2, 4):
        s_q, s_k, s_v, back, gains = finish(
            (g_q, g_k, g_v), part, jnp.pad(gains, ((0, 4), (0, 0)))
        )
    else:
        mine = part[: ctx // 2].astype(f32) + flip(part[ctx // 2 :], "row", 1).astype(f32)
        back = lax.ppermute(mine.astype(bf16), "row", [(2, 0), (3, 1)]).astype(f32)
        back = jnp.where(row < 2, mine + back, 0.0)
        gains = sum_all(gains)
        s_q, s_k, s_v = reduce_weights([g_q, g_k, g_v])
    da1 = own + back
    grad_tokens = dh1 + norm_back(n1, z1, gain_self, da1)

    return (
        layer_out,
        grad_tokens,
        grad_encoded,
        gains[0],
        s_q.T,
        s_k.T,
        s_v.T,
        s_o,
        gains[1],
        s_cq.T,
        s_ck.T,
        s_cv.T,
        s_co,
        gains[2],
        s_up.T,
        s_down,
        gains[3],
    )


def solution(mesh):
    rows = P(("dp", "col", "row"), None)
    down, across_ = P("col", "row"), P("row", "col")
    return jax.shard_map(
        layer,
        mesh=mesh,
        in_specs=(
            rows, rows, P(("dp", "col"), None), rows,
            P(), down, down, down, across_,
            P(), down, down, down, across_,
            P(), down, across_, P(),
        ),
        out_specs=(
            rows, rows, rows,
            P(), down, down, down, across_,
            P(), down, down, down, across_,
            P(), down, across_, P(),
        ),
        check_vma=False,
    )
```
